256 devices in a mesh: ctx: 64 (over x, z, core), tp: 4 (over y).
Axes of the slice: x: 4, y: 4, z: 8, core: 2. Of those that a mesh axis runs over, the one named last changes fastest.
Arguments:
- queries: bfloat16 [12288, 4096], P(('ctx', 'tp')), may hold values from -64 to 64
- keys: bfloat16 [12288, 512], P(('ctx', 'tp')), may hold values from -6 to 6
- values: bfloat16 [12288, 512], P(('ctx', 'tp')), may hold values from -6 to 6
- block_order: int32 [128], replicated, may hold values from 0 to 127, as said below
Outputs:
- attended: bfloat16 [12288, 4096], P(('ctx', 'tp'))
The draws below stay inside these ranges and needn't reach their ends.
Inputs may be any that keep to these rules, and one draw needn't show every extreme that they name: block_order is a permutation of the 128 blocks in which slots 2 c and 2 c + 1 hold blocks p and 127 - p for some p, in either order.
All inputs are finite; a program needn't handle non-finite values.
Results may differ from the reference program's by a relative error of at most 0.0055.
Values may be sent and summed in bfloat16 or wider, within the bound.
No kernel may reach another device: no remote copies, remote signals or barrier semaphores. Data moves between devices by JAX's collectives and lax.ppermute only.
A program may use at most 64 MiB of HBM per device.

```python
import jax
import jax.numpy as jnp
from jax import lax

QUERY_HEAD_COUNT = 32
KEY_VALUE_HEADS = 4
HEAD_SIZE = 128
TC = 192
BLOCK = 96
SEQUENCE_LENGTH = 12288
NBLK = 128


def shared_draw(key):
    unprocessed_keys = jnp.clip(jax.random.normal(jax.random.fold_in(key, 11), (SEQUENCE_LENGTH, KEY_VALUE_HEADS * HEAD_SIZE), jnp.float32), -6.0, 6.0)
    query_raw = jnp.clip(jax.random.normal(jax.random.fold_in(key, 12), (SEQUENCE_LENGTH, QUERY_HEAD_COUNT * HEAD_SIZE), jnp.float32), -6.0, 6.0)
    return (query_raw, unprocessed_keys)


def draw_queries(key, part):
    return shared_draw(key)[0].astype(jnp.bfloat16)


def draw_keys(key, part):
    return shared_draw(key)[1].astype(jnp.bfloat16)


def draw_block_order(key, part):
    half = NBLK // 2
    pairs = jax.random.permutation(jax.random.fold_in(key, 21), half).astype(jnp.int32)
    flips = jax.random.randint(jax.random.fold_in(key, 22), (half,), 0, 2)
    first = jnp.where(flips == 1, pairs, NBLK - 1 - pairs)
    second = NBLK - 1 - first
    return jnp.stack([first, second], axis=1).reshape(NBLK).astype(jnp.int32)


def block_levels(key, shape, shards, smallest, top_value):
    def one(axis_at, blocks):
        steps = jax.random.uniform(jax.random.fold_in(jax.random.fold_in(key, 6), axis_at), (blocks,), jnp.float32, smallest / len(shards), top_value / len(shards))
        return jnp.repeat(jnp.exp(steps), shape[axis_at] // blocks).reshape((-1,) + (1,) * (len(shape) - axis_at - 1))

    loudness = one(*shards[0])
    for cut in shards[1:]:
        loudness = loudness * one(*cut)
    return loudness


def normal_values(key, extent, scale, reach, split=(), kind=jnp.bfloat16):
    gain = block_levels(key, extent, split, -0.22, 0.18) if split else 1.0
    values = jax.random.normal(key, extent, jnp.float32) * scale * gain
    return jnp.minimum(jnp.maximum(values, -reach), reach).astype(kind)


def setup_inputs(seed: int = 0) -> dict:
    arg_keys = jax.random.split(jax.random.key(seed), 5)
    return {
        "queries": draw_queries(jax.random.fold_in(arg_keys[4], 71), 0),
        "keys": draw_keys(jax.random.fold_in(arg_keys[4], 71), 0),
        "values": normal_values(arg_keys[2], (SEQUENCE_LENGTH, KEY_VALUE_HEADS * HEAD_SIZE), 1.0, 6.0, ((0, 256),)),
        "block_order": draw_block_order(jax.random.fold_in(arg_keys[4], 71), 0),
    }


def positions(rows, block_order, span, block):
    owner = rows // span
    inner = rows % span
    index = (2 * owner + inner // block).astype(jnp.int32)
    table = jnp.arange(block_order.shape[0], dtype=jnp.int32)
    picked = jnp.sum(jnp.where(index[:, None] == table[None, :], block_order[None, :], 0), axis=1)
    return (picked * block + inner % block).astype(jnp.int32)


def reference(queries, keys, values, block_order):
    query_groups = QUERY_HEAD_COUNT // KEY_VALUE_HEADS
    pos = positions(jnp.arange(SEQUENCE_LENGTH, dtype=jnp.int32), block_order, TC, BLOCK)
    extent_total = max(d for d in range(1, min(SEQUENCE_LENGTH, 128) + 1) if SEQUENCE_LENGTH % d == 0)
    complete_keys = keys.astype(jnp.float32).reshape(SEQUENCE_LENGTH, KEY_VALUE_HEADS, HEAD_SIZE)
    complete_values = values.astype(jnp.float32).reshape(SEQUENCE_LENGTH, KEY_VALUE_HEADS, HEAD_SIZE)

    def one(index):
        begin_offset = (index * extent_total).astype(jnp.int32)
        query_rows = lax.dynamic_slice_in_dim(queries, begin_offset, extent_total, 0).astype(jnp.float32).reshape(extent_total, KEY_VALUE_HEADS, query_groups, HEAD_SIZE)
        rows_p = lax.dynamic_slice_in_dim(pos, begin_offset, extent_total, 0)
        scores = jnp.einsum("tkgd,skd->kgts", query_rows, complete_keys) * (HEAD_SIZE ** -0.5)
        visible = (pos[None, :] <= rows_p[:, None])[None, None]
        top = jnp.max(jnp.where(visible, scores, -1.0e30), axis=-1, keepdims=True)
        weights = jnp.where(visible, jnp.exp(scores - top), 0.0)
        denom = jnp.sum(weights, axis=-1)
        rounded = lax.optimization_barrier(weights.astype(jnp.bfloat16)).astype(jnp.float32)
        summed = jnp.einsum("kgts,skd->kgtd", rounded, complete_values)
        result = summed / denom[..., None]
        return jnp.transpose(result, (2, 0, 1, 3)).reshape(extent_total, QUERY_HEAD_COUNT * HEAD_SIZE).astype(jnp.bfloat16)

    blocks = lax.map(one, jnp.arange(SEQUENCE_LENGTH // extent_total, dtype=jnp.int32))
    return blocks.reshape(SEQUENCE_LENGTH, QUERY_HEAD_COUNT * HEAD_SIZE)
```

```python
import functools
import math

import jax
import jax.numpy as jnp
import numpy as np
from jax import lax
from jax.experimental import pallas as pl
from jax.experimental.pallas import tpu as pltpu
from jax.sharding import Mesh, PartitionSpec as P

QUERY_HEAD_COUNT = 32
KEY_VALUE_HEADS = 4
HEAD = 128
GROUP = QUERY_HEAD_COUNT // KEY_VALUE_HEADS
BLOCK = 96
LANES = GROUP * BLOCK
TILE = 8
WIDE = 256
NEG = -1e30
LOG2_SCALE = HEAD ** -0.5 * math.log2(math.e)
ROWS = HEAD + 8
NX, NZ = 4, 8


def shift(n, k):
    return [(i, (i + k) % n) for i in range(n)]


def ring(block, axis, n):
    pieces = [(0, block)]
    up = down = block
    for s in range(1, n // 2):
        up = lax.ppermute(up, axis, shift(n, 1))
        down = lax.ppermute(down, axis, shift(n, -1))
        pieces += [(-s, up), (s, down)]
    half = block.shape[0] // 2
    up = lax.ppermute(up[:half], axis, shift(n, 1))
    down = lax.ppermute(down[half:], axis, shift(n, -1))
    return pieces, (n // 2, up, down)


def attend_kernel(counts, first, *refs):
    cnt, idx, kpos, qpos, q_ref = refs[:5]
    at = 5 + len(counts)
    pieces = refs[5:at]
    if not first:
        own_in, other_in = refs[at : at + 2]
        at += 2
    own, other, kv, sems = refs[at : at + 4]
    copies, row = [], 0
    for i, n in enumerate(counts):
        copy = pltpu.make_async_copy(pieces[i], kv.at[pl.ds(row * BLOCK, n * BLOCK)], sems.at[i])
        copy.start()
        copies.append(copy)
        row += n
    for copy in copies:
        copy.wait()

    def query_block(base, before, state, b):
        qb = base + b
        n = cnt[qb]
        tiles = (n + TILE - 1) // TILE
        if first:
            state[b, 0:HEAD] = jnp.zeros((HEAD, LANES), jnp.float32)
            state[b, HEAD : HEAD + 1] = jnp.full((1, LANES), NEG, jnp.float32)
            state[b, HEAD + 1 : HEAD + 2] = jnp.zeros((1, LANES), jnp.float32)
        else:
            state[b] = before[b]

        def tile(t, masked):
            offs = [pl.multiple_of(idx[qb, t * TILE + j] * BLOCK, BLOCK) for j in range(TILE)]
            keys = jnp.concatenate([kv[pl.ds(f, BLOCK), 0:HEAD] for f in offs], 0)
            vals = jnp.concatenate([kv[pl.ds(f, BLOCK), HEAD : 2 * HEAD] for f in offs], 0)
            if masked:
                inner = lax.broadcasted_iota(jnp.int32, (BLOCK, 1), 0)
                kp = jnp.concatenate([inner + kpos[qb, t * TILE + j] * BLOCK for j in range(TILE)], 0)
            for c in range(LANES // WIDE):
                sl = slice(c * WIDE, (c + 1) * WIDE)
                s = lax.dot_general(
                    keys, q_ref[qb, :, sl], (((1,), (0,)), ((), ())), preferred_element_type=jnp.float32
                )
                if masked:
                    lane = lax.broadcasted_iota(jnp.int32, (1, WIDE), 1) + c * WIDE
                    s = jnp.where(kp <= lane % BLOCK + qpos[qb] * BLOCK, s, NEG)
                top = state[b, HEAD : HEAD + 1, sl]
                new = jnp.maximum(top, jnp.max(s, 0, keepdims=True))
                p = jnp.exp2((s - new) * LOG2_SCALE)
                decay = jnp.exp2((top - new) * LOG2_SCALE)
                state[b, HEAD : HEAD + 1, sl] = new
                state[b, HEAD + 1 : HEAD + 2, sl] = state[b, HEAD + 1 : HEAD + 2, sl] * decay + jnp.sum(
                    p, 0, keepdims=True
                )
                state[b, 0:HEAD, sl] = state[b, 0:HEAD, sl] * decay + lax.dot_general(
                    vals, p.astype(jnp.bfloat16), (((0,), (0,)), ((), ())), preferred_element_type=jnp.float32
                )

        def full(t, carry):
            tile(t, False)
            return carry

        lax.fori_loop(0, tiles - 1, full, 0)

        @pl.when(n > 0)
        def _():
            tile(tiles - 1, True)

    for base, state in ((0, own), (2, other)):
        before = None if first else (own_in if base == 0 else other_in)

        def body(b, carry):
            query_block(base, before, state, b)
            return carry

        lax.fori_loop(0, 2, body, 0)


def attend(tables, qpos, q_all, pieces, state):
    counts = [p.shape[0] // BLOCK for p in pieces]
    total = sum(counts)
    first = state is None
    smem = pl.BlockSpec(memory_space=pltpu.SMEM)
    vmem = pl.BlockSpec(memory_space=pltpu.VMEM)
    anywhere = pl.BlockSpec(memory_space=pl.ANY)
    held = [] if first else list(state)
    shape = jax.ShapeDtypeStruct((2, ROWS, LANES), jnp.float32)
    return pl.pallas_call(
        functools.partial(attend_kernel, counts, first),
        out_shape=(shape, shape),
        in_specs=[smem] * 4 + [vmem] + [anywhere] * len(pieces) + [vmem] * len(held),
        out_specs=(vmem, vmem),
        scratch_shapes=[
            pltpu.VMEM((total * BLOCK, 2 * HEAD), jnp.bfloat16),
            pltpu.SemaphoreType.DMA((len(pieces),)),
        ],
        compiler_params=pltpu.CompilerParams(vmem_limit_bytes=40 * 1024 * 1024),
        cost_estimate=pl.CostEstimate(
            flops=total * 2 * LANES * BLOCK * HEAD * 4,
            bytes_accessed=total * BLOCK * 4 * HEAD + 4 * ROWS * LANES * 4,
            transcendentals=total * 2 * LANES * BLOCK,
        ),
        name="attend",
    )(*tables, qpos, q_all, *pieces, *held)


def tables_of(qblk, kblk):
    nb = kblk.shape[0]
    here = jnp.arange(nb, dtype=jnp.int32)
    seen = kblk[None, :] <= qblk[:, None]
    rank = jnp.where(seen, jnp.where(kblk[None, :] == qblk[:, None], nb, here[None, :]), 2 * nb + here[None, :])
    place = jnp.sum(rank[:, None, :] < rank[:, :, None], 2)
    hit = place[:, :, None] == here[None, None, :]
    idx = jnp.sum(jnp.where(hit, here[None, :, None], 0), 1).astype(jnp.int32)
    kpos = jnp.sum(jnp.where(hit, kblk[None, :, None], 0), 1).astype(jnp.int32)
    pad = (-nb) % TILE
    if pad:
        idx = jnp.pad(idx, ((0, 0), (0, pad)))
        kpos = jnp.pad(kpos, ((0, 0), (0, pad)), constant_values=1 << 20)
    return jnp.sum(seen, 1).astype(jnp.int32), idx, kpos


def merge_kernel(mine, theirs, out):
    for b in range(2):
        m1, m2 = mine[b, HEAD : HEAD + 1], theirs[b, HEAD : HEAD + 1]
        top = jnp.maximum(m1, m2)
        w1 = jnp.exp2((m1 - top) * LOG2_SCALE)
        w2 = jnp.exp2((m2 - top) * LOG2_SCALE)
        denom = mine[b, HEAD + 1 : HEAD + 2] * w1 + theirs[b, HEAD + 1 : HEAD + 2] * w2
        o = (mine[b, 0:HEAD] * w1 + theirs[b, 0:HEAD] * w2) / denom
        rows = o.T.astype(jnp.bfloat16)
        for h in range(GROUP):
            out[b * BLOCK : (b + 1) * BLOCK, h * HEAD : (h + 1) * HEAD] = rows[h * BLOCK : (h + 1) * BLOCK]


def merge(mine, theirs):
    return pl.pallas_call(
        merge_kernel,
        out_shape=jax.ShapeDtypeStruct((2 * BLOCK, GROUP * HEAD), jnp.bfloat16),
        compiler_params=pltpu.CompilerParams(vmem_limit_bytes=16 * 1024 * 1024),
        name="merge",
    )(mine, theirs)


def lookup(block_order, index):
    table = jnp.arange(block_order.shape[0], dtype=jnp.int32)
    return jnp.sum(jnp.where(index[:, None] == table[None, :], block_order[None, :], 0), axis=1)


def shards(queries, keys, values, block_order):
    rows = queries.shape[0]
    x, z, c = lax.axis_index("x"), lax.axis_index("z"), lax.axis_index("c")
    pair = jnp.concatenate([keys.reshape(rows, 4, HEAD), values.reshape(rows, 4, HEAD)], 2).transpose(1, 0, 2)
    kv = lax.all_to_all(pair, "tp", split_axis=0, concat_axis=0, tiled=True).reshape(4 * rows, 2 * HEAD)

    def stored(places):
        dx, dz, slot = (np.asarray(v, np.int32) for v in zip(*places))
        return lookup(block_order, 2 * ((((x + dx) % NX) * NZ + (z + dz) % NZ) * 2 + c) + slot)

    def gather(block, slot, first, n1, second, n2, xfirst):
        got, (far, up, down) = ring(block, first, n1)
        offs1 = [o for o, _ in got] + [far]
        wide = jnp.concatenate([p for _, p in got] + [up, down], 0)
        got, (far, up, down) = ring(wide, second, n2)

        def ids(o2, offs):
            return [(o, o2, slot) if xfirst else (o2, o, slot) for o in offs]

        half = len(offs1) // 2
        pieces = [(p, ids(o, offs1)) for o, p in got]
        return pieces + [(up, ids(far, offs1[:half])), (down, ids(far, offs1[half:]))]

    part_a = gather(kv[:BLOCK], 0, "x", NX, "z", NZ, True)
    part_b = gather(kv[BLOCK:], 1, "z", NZ, "x", NX, False)

    q = lax.all_to_all(queries.reshape(rows, 4, GROUP * HEAD), "tp", split_axis=1, concat_axis=0, tiled=True)
    q_own = q.reshape(2, BLOCK, GROUP, HEAD).transpose(0, 3, 2, 1).reshape(2, HEAD, LANES)
    q_other = lax.ppermute(q_own, "c", shift(2, 1))
    q_all = jnp.concatenate([q_own, q_other], 0)
    ctx = (x * NZ + z) * 2
    own = np.asarray([1, 1, 0, 0], np.int32)
    core = own * c + (1 - own) * (1 - c)
    qpos = lookup(block_order, 2 * (ctx + core) + np.asarray([0, 1, 0, 1], np.int32))

    state = None
    for group in (part_a[:5] + part_b[:1], part_a[5:] + part_b[1:]):
        kblk = stored([i for _, ids in group for i in ids])
        state = attend(tables_of(qpos, kblk), qpos, q_all, [p for p, _ in group], state)
    theirs = lax.ppermute(state[1], "c", shift(2, 1))
    result = merge(state[0], theirs)
    return lax.all_to_all(result, "tp", split_axis=0, concat_axis=1, tiled=True)


def solution(mesh):
    cut = Mesh(mesh.devices.reshape(NX, NZ, 2, 4), ("x", "z", "c", "tp"))
    placed = P(("x", "z", "c", "tp"), None)
    return jax.shard_map(
        shards, mesh=cut, in_specs=(placed, placed, placed, P()), out_specs=placed, check_vma=False
    )
```

```python
import functools

import jax
import jax.numpy as jnp
import numpy as np
from jax import lax
from jax.experimental import pallas as pl
from jax.experimental.pallas import tpu as pltpu
from jax.sharding import Mesh, PartitionSpec as P

QUERY_HEAD_COUNT = 32
KEY_VALUE_HEADS = 4
HEAD = 128
GROUP = QUERY_HEAD_COUNT // KEY_VALUE_HEADS
BLOCK = 96
LANES = GROUP * BLOCK
TILE = 8
WIDE = 256
NEG = -1e30
SCALE = HEAD ** -0.5
ROWS = HEAD + 8
NX, NZ = 4, 8


def shift(n, k):
    return [(i, (i + k) % n) for i in range(n)]


def attend_kernel(counts, first, *refs):
    cnt, idx, kpos, qpos, q_own, q_other = refs[:6]
    at = 6 + len(counts)
    pieces = refs[6:at]
    if not first:
        before = refs[at : at + 2]
        at += 2
    own, other, kv, q_turned, work, sems = refs[at : at + 6]
    copies, row = [], 0
    for i, n in enumerate(counts):
        copy = pltpu.make_async_copy(pieces[i], kv.at[pl.ds(row * BLOCK, n * BLOCK)], sems.at[i])
        copy.start()
        copies.append(copy)
        row += n
    for copy in copies:
        copy.wait()

    def tile(qb, t, width, masked):
        offs = [pl.multiple_of(idx[qb, t * TILE + j] * BLOCK, BLOCK) for j in range(width)]
        keys = jnp.concatenate([kv[pl.ds(f, BLOCK), 0:HEAD] for f in offs], 0)
        vals = jnp.concatenate([kv[pl.ds(f, BLOCK), HEAD : 2 * HEAD] for f in offs], 0).T
        if masked:
            inner = lax.broadcasted_iota(jnp.int32, (BLOCK, 1), 0)
            kp = jnp.concatenate([inner + kpos[qb, t * TILE + j] * BLOCK for j in range(width)], 0)

        def logits(c):
            sl = slice(c * WIDE, (c + 1) * WIDE)
            s = jnp.dot(keys, q_turned[:, sl], preferred_element_type=jnp.float32)
            if masked:
                lane = lax.broadcasted_iota(jnp.int32, (1, WIDE), 1) + c * WIDE
                s = jnp.where(kp <= lane % BLOCK + qpos[qb] * BLOCK, s, NEG)
            return s

        def soften(c, s):
            sl = slice(c * WIDE, (c + 1) * WIDE)
            top = work[HEAD : HEAD + 1, sl]
            new = jnp.maximum(top, jnp.max(s, 0, keepdims=True))
            p = jnp.exp((s - new) * SCALE)
            decay = jnp.exp((top - new) * SCALE)
            work[HEAD : HEAD + 1, sl] = new
            work[HEAD + 1 : HEAD + 2, sl] = work[HEAD + 1 : HEAD + 2, sl] * decay + jnp.sum(p, 0, keepdims=True)
            return c, p.astype(jnp.bfloat16), decay

        def weigh(c, p, decay):
            sl = slice(c * WIDE, (c + 1) * WIDE)
            work[0:HEAD, sl] = work[0:HEAD, sl] * decay + jnp.dot(vals, p, preferred_element_type=jnp.float32)

        chunks = LANES // WIDE
        s, held = logits(0), None
        for c in range(chunks):
            following = logits(c + 1) if c + 1 < chunks else None
            now = soften(c, s)
            if held is not None:
                weigh(*held)
            held, s = now, following
        weigh(*held)

    def query_block(qb, carry):
        n = cnt[qb]
        full = lax.div(n - 1, TILE)
        rest = n - full * TILE
        if first:
            work[0:HEAD] = jnp.zeros((HEAD, LANES), jnp.float32)
            work[HEAD : HEAD + 1] = jnp.full((1, LANES), NEG, jnp.float32)
            work[HEAD + 1 : ROWS] = jnp.zeros((ROWS - HEAD - 1, LANES), jnp.float32)
        else:
            for side in range(2):

                @pl.when(qb // 2 == side)
                def _():
                    work[...] = before[side][qb % 2]

        for side, q_ref in ((0, q_own), (1, q_other)):

            @pl.when(qb // 2 == side)
            def _():
                start = pl.multiple_of(qb % 2 * BLOCK, BLOCK)
                heads = [q_ref[pl.ds(start, BLOCK), h * HEAD : (h + 1) * HEAD] for h in range(GROUP)]
                q_turned[...] = jnp.concatenate(heads, 0).T

        def step(t, carry):
            tile(qb, t, TILE, False)
            return carry

        lax.fori_loop(0, full, step, 0)

        @pl.when(rest > TILE // 2)
        def _():
            tile(qb, full, TILE, True)

        @pl.when((rest > 0) & (rest <= TILE // 2))
        def _():
            tile(qb, full, TILE // 2, True)

        for side, out in ((0, own), (1, other)):

            @pl.when(qb // 2 == side)
            def _():
                out[qb % 2] = work[...]

        return carry

    lax.fori_loop(0, 4, query_block, 0)


def attend(tables, qpos, q_own, q_other, pieces, state):
    counts = [p.shape[0] // BLOCK for p in pieces]
    total = sum(counts)
    first = state is None
    smem = pl.BlockSpec(memory_space=pltpu.SMEM)
    vmem = pl.BlockSpec(memory_space=pltpu.VMEM)
    anywhere = pl.BlockSpec(memory_space=pl.ANY)
    held = [] if first else list(state)
    shape = jax.ShapeDtypeStruct((2, ROWS, LANES), jnp.float32)
    return pl.pallas_call(
        functools.partial(attend_kernel, counts, first),
        out_shape=(shape, shape),
        in_specs=[smem] * 4 + [vmem] * 2 + [anywhere] * len(pieces) + [vmem] * len(held),
        out_specs=(vmem, vmem),
        scratch_shapes=[
            pltpu.VMEM((total * BLOCK, 2 * HEAD), jnp.bfloat16),
            pltpu.VMEM((HEAD, LANES), jnp.bfloat16),
            pltpu.VMEM((ROWS, LANES), jnp.float32),
            pltpu.SemaphoreType.DMA((len(pieces),)),
        ],
        compiler_params=pltpu.CompilerParams(vmem_limit_bytes=32 * 1024 * 1024),
        cost_estimate=pl.CostEstimate(
            flops=total * 2 * LANES * BLOCK * HEAD * 4,
            bytes_accessed=total * BLOCK * 4 * HEAD + 4 * ROWS * LANES * 4,
            transcendentals=total * 2 * LANES * BLOCK,
        ),
        name="attend",
    )(*tables, qpos, q_own, q_other, *pieces, *held)


def tables_of(qblk, kblk):
    nb = kblk.shape[1]
    here = jnp.arange(nb, dtype=jnp.int32)
    k, q = kblk[:, None, :], qblk[None, :, None]
    rank = jnp.where(k <= q, jnp.where(k == q, nb, here), 2 * nb + here)
    place = jnp.sum(rank[:, :, None, :] < rank[:, :, :, None], 3)
    hit = place[:, :, :, None] == here
    idx = jnp.sum(jnp.where(hit, here[:, None], 0), 2).astype(jnp.int32)
    kpos = jnp.sum(jnp.where(hit, k[:, :, :, None], 0), 2).astype(jnp.int32)
    return jnp.sum(k <= q, 2).astype(jnp.int32), idx, kpos


def merge_kernel(mine, theirs, out):
    for b in range(2):
        m1, m2 = mine[b, HEAD : HEAD + 1], theirs[b, HEAD : HEAD + 1]
        top = jnp.maximum(m1, m2)
        w1 = jnp.exp((m1 - top) * SCALE)
        w2 = jnp.exp((m2 - top) * SCALE)
        denom = mine[b, HEAD + 1 : HEAD + 2] * w1 + theirs[b, HEAD + 1 : HEAD + 2] * w2
        o = (mine[b, 0:HEAD] * w1 + theirs[b, 0:HEAD] * w2) / denom
        rows = o.T.astype(jnp.bfloat16)
        for h in range(GROUP):
            out[b * BLOCK : (b + 1) * BLOCK, h * HEAD : (h + 1) * HEAD] = rows[h * BLOCK : (h + 1) * BLOCK]


def merge(mine, theirs):
    return pl.pallas_call(
        merge_kernel,
        out_shape=jax.ShapeDtypeStruct((2 * BLOCK, GROUP * HEAD), jnp.bfloat16),
        compiler_params=pltpu.CompilerParams(vmem_limit_bytes=16 * 1024 * 1024),
        name="merge",
    )(mine, theirs)


def lookup(block_order, index):
    table = jnp.arange(block_order.shape[0], dtype=jnp.int32)
    return jnp.sum(jnp.where(index[:, None] == table[None, :], block_order[None, :], 0), axis=1)


def shards(queries, keys, values, block_order):
    rows = queries.shape[0]
    x, z, c = lax.axis_index("x"), lax.axis_index("z"), lax.axis_index("c")
    pair = jnp.concatenate([keys.reshape(rows, 4, HEAD), values.reshape(rows, 4, HEAD)], 2).transpose(1, 0, 2)
    spread = jnp.broadcast_to(pair[None], (NX, 4, rows, 2 * HEAD)).reshape(NX * 4, rows, 2 * HEAD)
    line = lax.all_to_all(spread, ("x", "tp"), split_axis=0, concat_axis=0, tiled=True).reshape(-1, 2 * HEAD)

    queries, line = lax.optimization_barrier((queries, line))
    q_own = lax.all_to_all(queries, "tp", split_axis=1, concat_axis=0, tiled=True)
    q_other = lax.ppermute(q_own, "c", shift(2, 1))

    ctx = (x * NZ + z) * 2
    own = np.asarray([1, 1, 0, 0], np.int32)
    core = own * c + (1 - own) * (1 - c)
    qpos = lookup(block_order, 2 * (ctx + core) + np.asarray([0, 1, 0, 1], np.int32))

    offsets = [(0, -1, 1), (-2, 2), (-3, 3), (NZ // 2,)]
    most = 2 * NX * max(len(o) for o in offsets)
    dz, dx, slot, real = (np.zeros((len(offsets), most), np.int32) for _ in range(4))
    for i, group in enumerate(offsets):
        for j, (o, xs, sl) in enumerate((o, xs, sl) for o in group for xs in range(NX) for sl in range(2)):
            dz[i, j], dx[i, j], slot[i, j], real[i, j] = o, xs, sl, 1
    stored = lookup(block_order, (2 * ((dx * NZ + (z + dz) % NZ) * 2 + c) + slot).reshape(-1)).reshape(dz.shape)
    cnt, idx, kpos = tables_of(qpos, jnp.where(real == 1, stored, 1 << 20))

    up, down = lax.ppermute(line, "z", shift(NZ, 1)), lax.ppermute(line, "z", shift(NZ, -1))
    pieces, state = [line, up, down], None
    for i in range(len(offsets)):
        if i < len(offsets) - 2:
            up, down = lax.ppermute(up, "z", shift(NZ, 1)), lax.ppermute(down, "z", shift(NZ, -1))
        elif i == len(offsets) - 2:
            half = line.shape[0] // 2
            up, down = lax.ppermute(up[:half], "z", shift(NZ, 1)), lax.ppermute(down[half:], "z", shift(NZ, -1))
        state = attend((cnt[i], idx[i], kpos[i]), qpos, q_own, q_other, pieces, state)
        if i < len(offsets) - 1:
            up, down, state = lax.optimization_barrier((up, down, state))
        pieces = [up, down]
    theirs = lax.ppermute(state[1], "c", shift(2, 1))
    result = merge(state[0], theirs)
    return lax.all_to_all(result, "tp", split_axis=0, concat_axis=1, tiled=True)


def solution(mesh):
    cut = Mesh(mesh.devices.reshape(NX, NZ, 2, 4), ("x", "z", "c", "tp"))
    placed = P(("x", "z", "c", "tp"), None)
    return jax.shard_map(
        shards, mesh=cut, in_specs=(placed, placed, placed, P()), out_specs=placed, check_vma=False
    )
```

```python
import functools
import math

import jax
import jax.numpy as jnp
import numpy as np
from jax import lax
from jax.experimental import pallas as pl
from jax.experimental.pallas import tpu as pltpu
from jax.sharding import Mesh, PartitionSpec as P


QUERY_HEAD_COUNT = 32
KEY_VALUE_HEADS = 4
HEAD = 128
GROUP = QUERY_HEAD_COUNT // KEY_VALUE_HEADS
BLOCK = 96
LANES = GROUP * BLOCK
TILE = 8
WIDE = 256
NEG = -1e30
LOG2_SCALE = HEAD ** -0.5 * math.log2(math.e)
TOO_LARGE = 2.0**60
ROWS = HEAD + 8
NX, NZ = 4, 8


def shift(n, k):
    return [(i, (i + k) % n) for i in range(n)]


def attend_kernel(counts, first, sides, *refs):
    cnt, seen, idx, kpos, qpos = refs[:5]
    at = 5 + len(sides)
    queries = refs[5:at]
    pieces = refs[at : at + len(counts)]
    at += len(counts)
    if not first:
        before = refs[at : at + len(sides)]
        at += len(sides)
    outs = refs[at : at + len(sides)]
    kv, q_turned, work, sems = refs[at + len(sides) :]
    copies, row = [], 0
    for i, n in enumerate(counts):
        copy = pltpu.make_async_copy(pieces[i], kv.at[pl.ds(row * BLOCK, n * BLOCK)], sems.at[i])
        copy.start()
        copies.append(copy)
        row += n
    for copy in copies:
        copy.wait()

    def fetch(qb, place, width):
        offs = [pl.multiple_of(idx[qb, place + j] * BLOCK, BLOCK) for j in range(width)]
        keys = jnp.concatenate([kv[pl.ds(f, BLOCK), 0:HEAD] for f in offs], 0)
        return keys, jnp.concatenate([kv[pl.ds(f, BLOCK), HEAD : 2 * HEAD] for f in offs], 0).T

    def pipelined(keys, mask, soften, weigh):
        chunks = LANES // WIDE

        def logits(c):
            s = jnp.dot(keys, q_turned[:, c * WIDE : (c + 1) * WIDE], preferred_element_type=jnp.float32)
            return mask(c, s)

        s, held = logits(0), None
        for c in range(chunks):
            following = logits(c + 1) if c + 1 < chunks else None
            now = soften(slice(c * WIDE, (c + 1) * WIDE), s)
            if held is not None:
                weigh(*held)
            held, s = now, following
        weigh(*held)

    def careful(qb, place):
        keys, vals = fetch(qb, place, 2)
        inner = lax.broadcasted_iota(jnp.int32, (BLOCK, 1), 0)
        kp = jnp.concatenate([inner + kpos[qb, place + j] * BLOCK for j in range(2)], 0)

        def mask(c, s):
            lane = lax.broadcasted_iota(jnp.int32, (1, WIDE), 1) + c * WIDE
            return jnp.where(kp <= lane % BLOCK + qpos[qb] * BLOCK, s, NEG)

        def soften(sl, s):
            top = work[HEAD : HEAD + 1, sl]
            new = jnp.maximum(top, jnp.max(s, 0, keepdims=True))
            p = jnp.exp2((s - new) * LOG2_SCALE)
            decay = jnp.exp2((top - new) * LOG2_SCALE)
            work[HEAD : HEAD + 1, sl] = new
            work[HEAD + 1 : HEAD + 2, sl] = work[HEAD + 1 : HEAD + 2, sl] * decay + jnp.sum(p, 0, keepdims=True)
            return sl, p.astype(jnp.bfloat16), decay

        def weigh(sl, p, decay):
            work[0:HEAD, sl] = work[0:HEAD, sl] * decay + jnp.dot(vals, p, preferred_element_type=jnp.float32)

        pipelined(keys, mask, soften, weigh)

    def quick(qb, place, width, left):
        keys, vals = fetch(qb, place, width)
        cut = (width - 1) * BLOCK

        def mask(c, s):
            if left is None:
                return s
            return jnp.concatenate([s[:cut], s[cut:] + jnp.where(left == width, 0.0, NEG)], 0)

        def soften(sl, s):
            p = jnp.exp2((s - work[HEAD : HEAD + 1, sl]) * LOG2_SCALE)
            work[HEAD + 1 : HEAD + 2, sl] += jnp.sum(p, 0, keepdims=True)
            return sl, p.astype(jnp.bfloat16)

        def weigh(sl, p):
            work[0:HEAD, sl] += jnp.dot(vals, p, preferred_element_type=jnp.float32)

        pipelined(keys, mask, soften, weigh)

    def query_block(b, carry):
        qb = 2 * sides[0] + b
        n = cnt[qb]
        lead = jnp.where((seen[qb] == 0) | (kpos[qb, 0] == qpos[qb]), jnp.minimum(n, 1), 0)
        full = lax.div(jnp.maximum(n - 2 * lead, 0), TILE)
        at = 2 * lead + full * TILE
        left = n - at

        def load():
            if first:
                work[0:HEAD] = jnp.zeros((HEAD, LANES), jnp.float32)
                work[HEAD : HEAD + 1] = jnp.full((1, LANES), NEG, jnp.float32)
                work[HEAD + 1 : ROWS] = jnp.zeros((ROWS - HEAD - 1, LANES), jnp.float32)
            else:
                for i in range(len(sides)):

                    @pl.when(b // 2 == i)
                    def _():
                        work[...] = before[i][b % 2]

        load()
        for i in range(len(sides)):

            @pl.when(b // 2 == i)
            def _():
                start = pl.multiple_of(b % 2 * BLOCK, BLOCK)
                heads = [queries[i][pl.ds(start, BLOCK), h * HEAD : (h + 1) * HEAD] for h in range(GROUP)]
                q_turned[...] = jnp.concatenate(heads, 0).T

        def slow(t, carry):
            careful(qb, t * 2)
            return carry

        def fast(t, carry):
            quick(qb, 2 * lead + t * TILE, TILE, None)
            return carry

        lax.fori_loop(0, lead, slow, 0)
        lax.fori_loop(0, full, fast, 0)
        for width in range(2, TILE + 1, 2):

            @pl.when((left == width) | (left == width - 1))
            def _():
                quick(qb, at, width, left)

        fine = jnp.max(jnp.where(work[HEAD + 1 : HEAD + 2] < TOO_LARGE, 0.0, 1.0)) == 0.0

        @pl.when(jnp.logical_not(fine))
        def _():
            load()
            lax.fori_loop(0, lax.div(n + 1, 2), slow, 0)

        for i in range(len(sides)):

            @pl.when(b // 2 == i)
            def _():
                outs[i][b % 2] = work[...]

        return carry

    lax.fori_loop(0, 2 * len(sides), query_block, 0)


def attend(tables, qpos, queries, pieces, state, sides=(0, 1)):
    counts = [p.shape[0] // BLOCK for p in pieces]
    total = sum(counts)
    first = state is None
    smem = pl.BlockSpec(memory_space=pltpu.SMEM)
    vmem = pl.BlockSpec(memory_space=pltpu.VMEM)
    anywhere = pl.BlockSpec(memory_space=pl.ANY)
    held = [] if first else [state[i] for i in sides]
    shape = jax.ShapeDtypeStruct((2, ROWS, LANES), jnp.float32)
    return pl.pallas_call(
        functools.partial(attend_kernel, counts, first, sides),
        out_shape=(shape,) * len(sides),
        in_specs=[smem] * 5 + [vmem] * len(sides) + [anywhere] * len(pieces) + [vmem] * len(held),
        out_specs=(vmem,) * len(sides),
        scratch_shapes=[
            pltpu.VMEM((total * BLOCK, 2 * HEAD), jnp.bfloat16),
            pltpu.VMEM((HEAD, LANES), jnp.bfloat16),
            pltpu.VMEM((ROWS, LANES), jnp.float32),
            pltpu.SemaphoreType.DMA((len(pieces),)),
        ],
        compiler_params=pltpu.CompilerParams(vmem_limit_bytes=32 * 1024 * 1024),
        cost_estimate=pl.CostEstimate(
            flops=total * len(sides) * LANES * BLOCK * HEAD * 4,
            bytes_accessed=total * BLOCK * 4 * HEAD + 4 * ROWS * LANES * 4,
            transcendentals=total * len(sides) * LANES * BLOCK,
        ),
        name="attend",
    )(*tables, qpos, *[queries[i] for i in sides], *pieces, *held)


def tables_of(qblk, kblk):
    nb = kblk.shape[1]
    here = jnp.arange(nb, dtype=jnp.int32)
    k, q = kblk[:, None, :], qblk[None, :, None]
    rank = jnp.where(k <= q, jnp.where(k == q, -1, here), 2 * nb + here)
    place = jnp.sum(rank[:, :, None, :] < rank[:, :, :, None], 3)
    hit = place[:, :, :, None] == here
    idx = jnp.sum(jnp.where(hit, here[:, None], 0), 2).astype(jnp.int32)
    kpos = jnp.sum(jnp.where(hit, k[:, :, :, None], 0), 2).astype(jnp.int32)
    cnt = jnp.sum(k <= q, 2).astype(jnp.int32)
    return cnt, jnp.cumsum(cnt, 0) - cnt, idx, kpos


def merge_kernel(mine, theirs, out):
    for b in range(2):
        m1, m2 = mine[b, HEAD : HEAD + 1], theirs[b, HEAD : HEAD + 1]
        top = jnp.maximum(m1, m2)
        w1 = jnp.exp2((m1 - top) * LOG2_SCALE)
        w2 = jnp.exp2((m2 - top) * LOG2_SCALE)
        denom = mine[b, HEAD + 1 : HEAD + 2] * w1 + theirs[b, HEAD + 1 : HEAD + 2] * w2
        o = (mine[b, 0:HEAD] * w1 + theirs[b, 0:HEAD] * w2) / denom
        rows = o.T.astype(jnp.bfloat16)
        for h in range(GROUP):
            out[b * BLOCK : (b + 1) * BLOCK, h * HEAD : (h + 1) * HEAD] = rows[h * BLOCK : (h + 1) * BLOCK]


def merge(mine, theirs):
    return pl.pallas_call(
        merge_kernel,
        out_shape=jax.ShapeDtypeStruct((2 * BLOCK, GROUP * HEAD), jnp.bfloat16),
        compiler_params=pltpu.CompilerParams(vmem_limit_bytes=16 * 1024 * 1024),
        name="merge",
    )(mine, theirs)


def lookup(block_order, index):
    table = jnp.arange(block_order.shape[0], dtype=jnp.int32)
    return jnp.sum(jnp.where(index[:, None] == table[None, :], block_order[None, :], 0), axis=1)


def attention(queries, keys, values, block_order):
    rows = queries.shape[0]
    x, z, c = lax.axis_index("x"), lax.axis_index("z"), lax.axis_index("c")
    pair = jnp.concatenate([keys.reshape(rows, 4, HEAD), values.reshape(rows, 4, HEAD)], 2).transpose(1, 0, 2)
    spread = jnp.broadcast_to(pair[None], (NX, 4, rows, 2 * HEAD)).reshape(NX * 4, rows, 2 * HEAD)
    line = lax.all_to_all(spread, ("x", "tp"), split_axis=0, concat_axis=0, tiled=True).reshape(-1, 2 * HEAD)

    q_own = lax.all_to_all(queries, "tp", split_axis=1, concat_axis=0, tiled=True)
    q_other = lax.ppermute(q_own, "c", shift(2, 1))

    ctx = (x * NZ + z) * 2
    own = np.asarray([1, 1, 0, 0], np.int32)
    core = own * c + (1 - own) * (1 - c)
    qpos = lookup(block_order, 2 * (ctx + core) + np.asarray([0, 1, 0, 1], np.int32))

    offsets = [(0, -1, 1), (-2, 2), (-3, 3), (NZ // 2,)]
    most = 2 * NX * max(len(o) for o in offsets)
    dz, dx, slot, real = (np.zeros((len(offsets), most), np.int32) for _ in range(4))
    for i, group in enumerate(offsets):
        for j, (o, xs, sl) in enumerate((o, xs, sl) for o in group for xs in range(NX) for sl in range(2)):
            dz[i, j], dx[i, j], slot[i, j], real[i, j] = o, xs, sl, 1
    stored = lookup(block_order, (2 * ((dx * NZ + (z + dz) % NZ) * 2 + c) + slot).reshape(-1)).reshape(dz.shape)
    tables = tables_of(qpos, jnp.where(real == 1, stored, 1 << 20))

    up, down = lax.ppermute(line, "z", shift(NZ, 1)), lax.ppermute(line, "z", shift(NZ, -1))
    pieces, state = [line, up, down], None
    for i in range(len(offsets)):
        if i < len(offsets) - 2:
            up, down = lax.ppermute(up, "z", shift(NZ, 1)), lax.ppermute(down, "z", shift(NZ, -1))
        elif i == len(offsets) - 2:
            half = line.shape[0] // 2
            up, down = lax.ppermute(up[:half], "z", shift(NZ, 1)), lax.ppermute(down[half:], "z", shift(NZ, -1))
        part = [t[i] for t in tables]
        if i < len(offsets) - 1:
            state = attend(part, qpos, (q_own, q_other), pieces, state)
            up, down, state = lax.optimization_barrier((up, down, state))
            pieces = [up, down]
    (sent,) = attend(part, qpos, (q_own, q_other), pieces, state, (1,))
    theirs = lax.ppermute(sent, "c", shift(2, 1))
    (mine,) = attend(part, qpos, (q_own, q_other), pieces, state, (0,))
    result = merge(mine, theirs)
    return lax.all_to_all(result, "tp", split_axis=0, concat_axis=1, tiled=True)


def solution(mesh):
    cut = Mesh(mesh.devices.reshape(NX, NZ, 2, 4), ("x", "z", "c", "tp"))
    placed = P(("x", "z", "c", "tp"), None)
    return jax.shard_map(attention, mesh=cut, in_specs=(placed, placed, placed, P()), out_specs=placed, check_vma=False)
```

```python
import functools
import math

import jax
import jax.numpy as jnp
import numpy as np
from jax import lax
from jax.experimental import pallas as pl
from jax.experimental.pallas import tpu as pltpu
from jax.sharding import Mesh, PartitionSpec as P


QUERY_HEAD_COUNT = 32
KEY_VALUE_HEADS = 4
HEAD = 128
GROUP = QUERY_HEAD_COUNT // KEY_VALUE_HEADS
BLOCK = 96
LANES = GROUP * BLOCK
TILE = 8
WIDE = 256
NEG = -1e30
LOG2_SCALE = HEAD ** -0.5 * math.log2(math.e)
TOO_LARGE = 2.0**60
ROWS = HEAD + 8
NX, NZ = 4, 8


def shift(n, k):
    return [(i, (i + k) % n) for i in range(n)]


def attend_kernel(counts, first, sides, *refs):
    cnt, seen, idx, kpos, qpos = refs[:5]
    at = 5 + len(sides)
    queries = refs[5:at]
    pieces = refs[at : at + len(counts)]
    at += len(counts)
    if not first:
        before = refs[at : at + len(sides)]
        at += len(sides)
    outs = refs[at : at + len(sides)]
    kv, q_turned, work = refs[at + len(sides) :]
    row = 0
    for piece, n in zip(pieces, counts):
        kv[row : row + n * BLOCK] = piece[...]
        row += n * BLOCK

    def fetch(qb, place, width):
        offs = [pl.multiple_of(idx[qb, place + j] * BLOCK, BLOCK) for j in range(width)]
        keys = jnp.concatenate([kv[pl.ds(f, BLOCK), 0:HEAD] for f in offs], 0)
        return keys, jnp.concatenate([kv[pl.ds(f, BLOCK), HEAD : 2 * HEAD] for f in offs], 0).T

    def pipelined(keys, mask, soften, weigh):
        chunks = LANES // WIDE

        def logits(c):
            s = jnp.dot(keys, q_turned[:, c * WIDE : (c + 1) * WIDE], preferred_element_type=jnp.float32)
            return mask(c, s)

        s, held = logits(0), None
        for c in range(chunks):
            following = logits(c + 1) if c + 1 < chunks else None
            now = soften(slice(c * WIDE, (c + 1) * WIDE), s)
            if held is not None:
                weigh(*held)
            held, s = now, following
        weigh(*held)

    def careful(qb, place):
        keys, vals = fetch(qb, place, 2)
        inner = lax.broadcasted_iota(jnp.int32, (BLOCK, 1), 0)
        kp = jnp.concatenate([inner + kpos[qb, place + j] * BLOCK for j in range(2)], 0)

        def mask(c, s):
            lane = lax.broadcasted_iota(jnp.int32, (1, WIDE), 1) + c * WIDE
            return jnp.where(kp <= lane % BLOCK + qpos[qb] * BLOCK, s, NEG)

        def soften(sl, s):
            top = work[HEAD : HEAD + 1, sl]
            new = jnp.maximum(top, jnp.max(s, 0, keepdims=True))
            p = jnp.exp2((s - new) * LOG2_SCALE)
            decay = jnp.exp2((top - new) * LOG2_SCALE)
            work[HEAD : HEAD + 1, sl] = new
            work[HEAD + 1 : HEAD + 2, sl] = work[HEAD + 1 : HEAD + 2, sl] * decay + jnp.sum(p, 0, keepdims=True)
            return sl, p.astype(jnp.bfloat16), decay

        def weigh(sl, p, decay):
            work[0:HEAD, sl] = work[0:HEAD, sl] * decay + jnp.dot(vals, p, preferred_element_type=jnp.float32)

        pipelined(keys, mask, soften, weigh)

    def quick(qb, place, width, left):
        keys, vals = fetch(qb, place, width)
        cut = (width - 1) * BLOCK

        def mask(c, s):
            if left is None:
                return s
            return jnp.concatenate([s[:cut], s[cut:] + jnp.where(left == width, 0.0, NEG)], 0)

        def soften(sl, s):
            p = jnp.exp2((s - work[HEAD : HEAD + 1, sl]) * LOG2_SCALE)
            work[HEAD + 1 : HEAD + 2, sl] += jnp.sum(p, 0, keepdims=True)
            return sl, p.astype(jnp.bfloat16)

        def weigh(sl, p):
            work[0:HEAD, sl] += jnp.dot(vals, p, preferred_element_type=jnp.float32)

        pipelined(keys, mask, soften, weigh)

    def query_block(b, carry):
        qb = 2 * sides[0] + b
        n = cnt[qb]
        lead = jnp.where((seen[qb] == 0) | (kpos[qb, 0] == qpos[qb]), jnp.minimum(n, 1), 0)
        full = lax.div(jnp.maximum(n - 2 * lead, 0), TILE)
        at = 2 * lead + full * TILE
        left = n - at

        def load():
            if first:
                work[0:HEAD] = jnp.zeros((HEAD, LANES), jnp.float32)
                work[HEAD : HEAD + 1] = jnp.full((1, LANES), NEG, jnp.float32)
                work[HEAD + 1 : ROWS] = jnp.zeros((ROWS - HEAD - 1, LANES), jnp.float32)
            else:
                for i in range(len(sides)):

                    @pl.when(b // 2 == i)
                    def _():
                        work[...] = before[i][b % 2]

        load()
        for i in range(len(sides)):

            @pl.when(b // 2 == i)
            def _():
                start = pl.multiple_of(b % 2 * BLOCK, BLOCK)
                heads = [queries[i][pl.ds(start, BLOCK), h * HEAD : (h + 1) * HEAD] for h in range(GROUP)]
                q_turned[...] = jnp.concatenate(heads, 0).T

        def slow(t, carry):
            careful(qb, t * 2)
            return carry

        def fast(t, carry):
            quick(qb, 2 * lead + t * TILE, TILE, None)
            return carry

        lax.fori_loop(0, lead, slow, 0)
        lax.fori_loop(0, full, fast, 0)
        for width in range(2, TILE + 1, 2):

            @pl.when((left == width) | (left == width - 1))
            def _():
                quick(qb, at, width, left)

        fine = jnp.max(jnp.where(work[HEAD + 1 : HEAD + 2] < TOO_LARGE, 0.0, 1.0)) == 0.0

        @pl.when(jnp.logical_not(fine))
        def _():
            load()
            lax.fori_loop(0, lax.div(n + 1, 2), slow, 0)

        for i in range(len(sides)):

            @pl.when(b // 2 == i)
            def _():
                outs[i][b % 2] = work[...]

        return carry

    lax.fori_loop(0, 2 * len(sides), query_block, 0)


def attend(tables, qpos, queries, pieces, state, sides=(0, 1)):
    counts = [p.shape[0] // BLOCK for p in pieces]
    total = sum(counts)
    first = state is None
    smem = pl.BlockSpec(memory_space=pltpu.SMEM)
    vmem = pl.BlockSpec(memory_space=pltpu.VMEM)
    held = [] if first else [state[i] for i in sides]
    shape = jax.ShapeDtypeStruct((2, ROWS, LANES), jnp.float32)
    return pl.pallas_call(
        functools.partial(attend_kernel, counts, first, sides),
        out_shape=(shape,) * len(sides),
        in_specs=[smem] * 5 + [vmem] * len(sides) + [vmem] * len(pieces) + [vmem] * len(held),
        out_specs=(vmem,) * len(sides),
        scratch_shapes=[
            pltpu.VMEM((total * BLOCK, 2 * HEAD), jnp.bfloat16),
            pltpu.VMEM((HEAD, LANES), jnp.bfloat16),
            pltpu.VMEM((ROWS, LANES), jnp.float32),
        ],
        compiler_params=pltpu.CompilerParams(vmem_limit_bytes=32 * 1024 * 1024),
        cost_estimate=pl.CostEstimate(
            flops=total * len(sides) * LANES * BLOCK * HEAD * 4,
            bytes_accessed=total * BLOCK * 4 * HEAD + 4 * ROWS * LANES * 4,
            transcendentals=total * len(sides) * LANES * BLOCK,
        ),
        name="attend",
    )(*tables, qpos, *[queries[i] for i in sides], *pieces, *held)


def tables_of(qblk, kblk):
    nb = kblk.shape[1]
    here = jnp.arange(nb, dtype=jnp.int32)
    k, q = kblk[:, None, :], qblk[None, :, None]
    rank = jnp.where(k <= q, jnp.where(k == q, -1, here), 2 * nb + here)
    place = jnp.sum(rank[:, :, None, :] < rank[:, :, :, None], 3)
    hit = place[:, :, :, None] == here
    idx = jnp.sum(jnp.where(hit, here[:, None], 0), 2).astype(jnp.int32)
    kpos = jnp.sum(jnp.where(hit, k[:, :, :, None], 0), 2).astype(jnp.int32)
    cnt = jnp.sum(k <= q, 2).astype(jnp.int32)
    return cnt, jnp.cumsum(cnt, 0) - cnt, idx, kpos


def merge_kernel(me, mine, theirs, *refs):
    outs, rows_ref = refs[:4], refs[4]
    for b in range(2):
        m1, m2 = mine[b, HEAD : HEAD + 1], theirs[b, HEAD : HEAD + 1]
        top = jnp.maximum(m1, m2)
        w1 = jnp.exp2((m1 - top) * LOG2_SCALE)
        w2 = jnp.exp2((m2 - top) * LOG2_SCALE)
        denom = mine[b, HEAD + 1 : HEAD + 2] * w1 + theirs[b, HEAD + 1 : HEAD + 2] * w2
        o = (mine[b, 0:HEAD] * w1 + theirs[b, 0:HEAD] * w2) / denom
        rows = o.T.astype(jnp.bfloat16)
        for h in range(GROUP):
            rows_ref[b * BLOCK : (b + 1) * BLOCK, h * HEAD : (h + 1) * HEAD] = rows[h * BLOCK : (h + 1) * BLOCK]
    count = outs[0].shape[0]
    for k, out in enumerate(outs):
        out[...] = rows_ref[pl.ds(pl.multiple_of(lax.rem(me[0] + k, 4) * count, count), count)]


def merge(me, mine, theirs, rows):
    vmem = pl.BlockSpec(memory_space=pltpu.VMEM)
    return pl.pallas_call(
        merge_kernel,
        out_shape=(jax.ShapeDtypeStruct((rows, GROUP * HEAD), jnp.bfloat16),) * 4,
        in_specs=[pl.BlockSpec(memory_space=pltpu.SMEM), vmem, vmem],
        out_specs=(vmem,) * 4,
        scratch_shapes=[pltpu.VMEM((2 * BLOCK, GROUP * HEAD), jnp.bfloat16)],
        compiler_params=pltpu.CompilerParams(vmem_limit_bytes=16 * 1024 * 1024),
        name="merge",
    )(me, mine, theirs)


def join_kernel(me, *refs):
    out = refs[4]
    width = GROUP * HEAD
    for k in range(4):
        out[:, pl.ds(pl.multiple_of(lax.rem(me[0] + 4 - k, 4) * width, width), width)] = refs[k][...]


def join(me, parts):
    vmem = pl.BlockSpec(memory_space=pltpu.VMEM)
    return pl.pallas_call(
        join_kernel,
        out_shape=jax.ShapeDtypeStruct((parts[0].shape[0], 4 * GROUP * HEAD), jnp.bfloat16),
        in_specs=[pl.BlockSpec(memory_space=pltpu.SMEM)] + [vmem] * 4,
        out_specs=vmem,
        compiler_params=pltpu.CompilerParams(vmem_limit_bytes=8 * 1024 * 1024),
        name="join",
    )(me, *parts)


def spread_kernel(keys, values, out):
    for h in range(KEY_VALUE_HEADS):
        sl = slice(h * HEAD, (h + 1) * HEAD)
        k, v = keys[:, sl], values[:, sl]
        for i in range(NX):
            out[i * KEY_VALUE_HEADS + h, :, 0:HEAD] = k
            out[i * KEY_VALUE_HEADS + h, :, HEAD : 2 * HEAD] = v


def spread(keys, values):
    return pl.pallas_call(
        spread_kernel,
        out_shape=jax.ShapeDtypeStruct((NX * KEY_VALUE_HEADS, keys.shape[0], 2 * HEAD), jnp.bfloat16),
        compiler_params=pltpu.CompilerParams(vmem_limit_bytes=4 * 1024 * 1024),
        name="spread",
    )(keys, values)


def lookup(block_order, index):
    table = jnp.arange(block_order.shape[0], dtype=jnp.int32)
    return jnp.sum(jnp.where(index[:, None] == table[None, :], block_order[None, :], 0), axis=1)


def attention(queries, keys, values, block_order):
    rows = queries.shape[0]
    x, z, c = lax.axis_index("x"), lax.axis_index("z"), lax.axis_index("c")
    line = lax.all_to_all(spread(keys, values), ("x", "tp"), split_axis=0, concat_axis=0, tiled=True)
    line = line.reshape(-1, 2 * HEAD)

    q_own = lax.all_to_all(queries, "tp", split_axis=1, concat_axis=0, tiled=True)
    q_other = lax.ppermute(q_own, "c", shift(2, 1))

    ctx = (x * NZ + z) * 2
    own = np.asarray([1, 1, 0, 0], np.int32)
    core = own * c + (1 - own) * (1 - c)
    qpos = lookup(block_order, 2 * (ctx + core) + np.asarray([0, 1, 0, 1], np.int32))

    offsets = [(0, -1, 1), (-2, 2), (-3, 3), (NZ // 2,)]
    most = 2 * NX * max(len(o) for o in offsets)
    dz, dx, slot, real = (np.zeros((len(offsets), most), np.int32) for _ in range(4))
    for i, group in enumerate(offsets):
        for j, (o, xs, sl) in enumerate((o, xs, sl) for o in group for xs in range(NX) for sl in range(2)):
            dz[i, j], dx[i, j], slot[i, j], real[i, j] = o, xs, sl, 1
    stored = lookup(block_order, (2 * ((dx * NZ + (z + dz) % NZ) * 2 + c) + slot).reshape(-1)).reshape(dz.shape)
    tables = tables_of(qpos, jnp.where(real == 1, stored, 1 << 20))

    up, down = lax.ppermute(line, "z", shift(NZ, 1)), lax.ppermute(line, "z", shift(NZ, -1))
    pieces, state = [line, up, down], None
    for i in range(len(offsets)):
        if i < len(offsets) - 2:
            up, down = lax.ppermute(up, "z", shift(NZ, 1)), lax.ppermute(down, "z", shift(NZ, -1))
        elif i == len(offsets) - 2:
            half = line.shape[0] // 2
            up, down = lax.ppermute(up[:half], "z", shift(NZ, 1)), lax.ppermute(down[half:], "z", shift(NZ, -1))
        part = [t[i] for t in tables]
        if i < len(offsets) - 1:
            state = attend(part, qpos, (q_own, q_other), pieces, state)
            up, down, state = lax.optimization_barrier((up, down, state))
            pieces = [up, down]
    (sent,) = attend(part, qpos, (q_own, q_other), pieces, state, (1,))
    theirs = lax.ppermute(sent, "c", shift(2, 1))
    (mine,) = attend(part, qpos, (q_own, q_other), pieces, state, (0,))
    me = lax.axis_index("tp").reshape(1)
    parts = merge(me, mine, theirs, rows)
    parts = [parts[0]] + [lax.ppermute(parts[k], "tp", shift(4, k)) for k in range(1, 4)]
    return join(me, parts)


def solution(mesh):
    cut = Mesh(mesh.devices.reshape(NX, NZ, 2, 4), ("x", "z", "c", "tp"))
    placed = P(("x", "z", "c", "tp"), None)
    return jax.shard_map(attention, mesh=cut, in_specs=(placed, placed, placed, P()), out_specs=placed, check_vma=False)
```

```python
import functools
import math

import jax
import jax.numpy as jnp
import numpy as np
from jax import lax
from jax.experimental import pallas as pl
from jax.experimental.pallas import tpu as pltpu
from jax.sharding import Mesh, PartitionSpec as P


QUERY_HEAD_COUNT = 32
KEY_VALUE_HEADS = 4
HEAD = 128
GROUP = QUERY_HEAD_COUNT // KEY_VALUE_HEADS
BLOCK = 96
LANES = GROUP * BLOCK
TILE = 8
WIDE = 256
NEG = -1e30
LOG2_SCALE = HEAD ** -0.5 * math.log2(math.e)
TOO_LARGE = 2.0**60
ROWS = HEAD + 8
NX, NZ = 4, 8


def shift(n, k):
    return [(i, (i + k) % n) for i in range(n)]


def attend_kernel(counts, first, sides, *refs):
    cnt, seen, idx, kpos, qpos = refs[:5]
    at = 5 + len(sides)
    queries = refs[5:at]
    pieces = refs[at : at + len(counts)]
    at += len(counts)
    if not first:
        before = refs[at : at + len(sides)]
        at += len(sides)
    outs = refs[at : at + len(sides)]
    kv, q_turned, work = refs[at + len(sides) :]
    row = 0
    for piece, n in zip(pieces, counts):
        kv[row : row + n * BLOCK] = piece[...]
        row += n * BLOCK

    def fetch(qb, place, width):
        offs = [pl.multiple_of(idx[qb, place + j] * BLOCK, BLOCK) for j in range(width)]
        keys = jnp.concatenate([kv[pl.ds(f, BLOCK), 0:HEAD] for f in offs], 0)
        return keys, jnp.concatenate([kv[pl.ds(f, BLOCK), HEAD : 2 * HEAD] for f in offs], 0).T

    def pipelined(keys, mask, soften, weigh):
        chunks = LANES // WIDE

        def logits(c):
            s = jnp.dot(keys, q_turned[:, c * WIDE : (c + 1) * WIDE], preferred_element_type=jnp.float32)
            return mask(c, s)

        s, held = logits(0), None
        for c in range(chunks):
            following = logits(c + 1) if c + 1 < chunks else None
            now = soften(slice(c * WIDE, (c + 1) * WIDE), s)
            if held is not None:
                weigh(*held)
            held, s = now, following
        weigh(*held)

    def careful(qb, place):
        keys, vals = fetch(qb, place, 2)
        inner = lax.broadcasted_iota(jnp.int32, (BLOCK, 1), 0)
        kp = jnp.concatenate([inner + kpos[qb, place + j] * BLOCK for j in range(2)], 0)

        def mask(c, s):
            lane = lax.broadcasted_iota(jnp.int32, (1, WIDE), 1) + c * WIDE
            return jnp.where(kp <= lane % BLOCK + qpos[qb] * BLOCK, s, NEG)

        def soften(sl, s):
            top = work[HEAD : HEAD + 1, sl]
            new = jnp.maximum(top, jnp.max(s, 0, keepdims=True))
            p = jnp.exp2((s - new) * LOG2_SCALE)
            decay = jnp.exp2((top - new) * LOG2_SCALE)
            work[HEAD : HEAD + 1, sl] = new
            work[HEAD + 1 : HEAD + 2, sl] = work[HEAD + 1 : HEAD + 2, sl] * decay + jnp.sum(p, 0, keepdims=True)
            return sl, p.astype(jnp.bfloat16), decay

        def weigh(sl, p, decay):
            work[0:HEAD, sl] = work[0:HEAD, sl] * decay + jnp.dot(vals, p, preferred_element_type=jnp.float32)

        pipelined(keys, mask, soften, weigh)

    def quick(qb, place, width, left):
        keys, vals = fetch(qb, place, width)
        cut = (width - 1) * BLOCK

        def mask(c, s):
            if left is None:
                return s
            return jnp.concatenate([s[:cut], s[cut:] + jnp.where(left == width, 0.0, NEG)], 0)

        def soften(sl, s):
            p = jnp.exp2((s - work[HEAD : HEAD + 1, sl]) * LOG2_SCALE)
            work[HEAD + 1 : HEAD + 2, sl] += jnp.sum(p, 0, keepdims=True)
            return sl, p.astype(jnp.bfloat16)

        def weigh(sl, p):
            work[0:HEAD, sl] += jnp.dot(vals, p, preferred_element_type=jnp.float32)

        pipelined(keys, mask, soften, weigh)

    def query_block(b, carry):
        qb = 2 * sides[0] + b
        n = cnt[qb]
        lead = jnp.where((seen[qb] == 0) | (kpos[qb, 0] == qpos[qb]), jnp.minimum(n, 1), 0)
        full = lax.div(jnp.maximum(n - 2 * lead, 0), TILE)
        at = 2 * lead + full * TILE
        left = n - at

        def load():
            if first:
                work[0:HEAD] = jnp.zeros((HEAD, LANES), jnp.float32)
                work[HEAD : HEAD + 1] = jnp.full((1, LANES), NEG, jnp.float32)
                work[HEAD + 1 : ROWS] = jnp.zeros((ROWS - HEAD - 1, LANES), jnp.float32)
            else:
                for i in range(len(sides)):

                    @pl.when(b // 2 == i)
                    def _():
                        work[...] = before[i][b % 2]

        load()
        for i in range(len(sides)):

            @pl.when(b // 2 == i)
            def _():
                start = pl.multiple_of(b % 2 * BLOCK, BLOCK)
                heads = [queries[i][pl.ds(start, BLOCK), h * HEAD : (h + 1) * HEAD] for h in range(GROUP)]
                q_turned[...] = jnp.concatenate(heads, 0).T

        def slow(t, carry):
            careful(qb, t * 2)
            return carry

        def fast(t, carry):
            quick(qb, 2 * lead + t * TILE, TILE, None)
            return carry

        lax.fori_loop(0, lead, slow, 0)
        lax.fori_loop(0, full, fast, 0)
        for width in range(2, TILE + 1, 2):

            @pl.when((left == width) | (left == width - 1))
            def _():
                quick(qb, at, width, left)

        fine = jnp.max(jnp.where(work[HEAD + 1 : HEAD + 2] < TOO_LARGE, 0.0, 1.0)) == 0.0

        @pl.when(jnp.logical_not(fine))
        def _():
            load()
            lax.fori_loop(0, lax.div(n + 1, 2), slow, 0)

        for i in range(len(sides)):

            @pl.when(b // 2 == i)
            def _():
                outs[i][b % 2] = work[...]

        return carry

    lax.fori_loop(0, 2 * len(sides), query_block, 0)


def attend(tables, qpos, queries, pieces, state, sides=(0, 1)):
    counts = [p.shape[0] // BLOCK for p in pieces]
    total = sum(counts)
    first = state is None
    smem = pl.BlockSpec(memory_space=pltpu.SMEM)
    vmem = pl.BlockSpec(memory_space=pltpu.VMEM)
    held = [] if first else [state[i] for i in sides]
    shape = jax.ShapeDtypeStruct((2, ROWS, LANES), jnp.float32)
    return pl.pallas_call(
        functools.partial(attend_kernel, counts, first, sides),
        out_shape=(shape,) * len(sides),
        in_specs=[smem] * 5 + [vmem] * len(sides) + [vmem] * len(pieces) + [vmem] * len(held),
        out_specs=(vmem,) * len(sides),
        scratch_shapes=[
            pltpu.VMEM((total * BLOCK, 2 * HEAD), jnp.bfloat16),
            pltpu.VMEM((HEAD, LANES), jnp.bfloat16),
            pltpu.VMEM((ROWS, LANES), jnp.float32),
        ],
        compiler_params=pltpu.CompilerParams(vmem_limit_bytes=32 * 1024 * 1024),
        cost_estimate=pl.CostEstimate(
            flops=total * len(sides) * LANES * BLOCK * HEAD * 4,
            bytes_accessed=total * BLOCK * 4 * HEAD + 4 * ROWS * LANES * 4,
            transcendentals=total * len(sides) * LANES * BLOCK,
        ),
        name="attend",
    )(*tables, qpos, *[queries[i] for i in sides], *pieces, *held)


def tables_of(qblk, kblk):
    nb = kblk.shape[1]
    here = jnp.arange(nb, dtype=jnp.int32)
    k, q = kblk[:, None, :], qblk[None, :, None]
    rank = jnp.where(k <= q, jnp.where(k == q, -1, here), 2 * nb + here)
    place = jnp.sum(rank[:, :, None, :] < rank[:, :, :, None], 3)
    hit = place[:, :, :, None] == here
    idx = jnp.sum(jnp.where(hit, here[:, None], 0), 2).astype(jnp.int32)
    kpos = jnp.sum(jnp.where(hit, k[:, :, :, None], 0), 2).astype(jnp.int32)
    cnt = jnp.sum(k <= q, 2).astype(jnp.int32)
    return cnt, jnp.cumsum(cnt, 0) - cnt, idx, kpos


def merge_kernel(me, mine, theirs, *refs):
    outs, rows_ref = refs[:4], refs[4]
    for b in range(2):
        m1, m2 = mine[b, HEAD : HEAD + 1], theirs[b, HEAD : HEAD + 1]
        top = jnp.maximum(m1, m2)
        w1 = jnp.exp2((m1 - top) * LOG2_SCALE)
        w2 = jnp.exp2((m2 - top) * LOG2_SCALE)
        denom = mine[b, HEAD + 1 : HEAD + 2] * w1 + theirs[b, HEAD + 1 : HEAD + 2] * w2
        o = (mine[b, 0:HEAD] * w1 + theirs[b, 0:HEAD] * w2) / denom
        rows = o.T.astype(jnp.bfloat16)
        for h in range(GROUP):
            rows_ref[b * BLOCK : (b + 1) * BLOCK, h * HEAD : (h + 1) * HEAD] = rows[h * BLOCK : (h + 1) * BLOCK]
    count = outs[0].shape[0]
    for k, out in enumerate(outs):
        out[...] = rows_ref[pl.ds(pl.multiple_of(lax.rem(me[0] + k, 4) * count, count), count)]


def merge(me, mine, theirs, rows):
    vmem = pl.BlockSpec(memory_space=pltpu.VMEM)
    return pl.pallas_call(
        merge_kernel,
        out_shape=(jax.ShapeDtypeStruct((rows, GROUP * HEAD), jnp.bfloat16),) * 4,
        in_specs=[pl.BlockSpec(memory_space=pltpu.SMEM), vmem, vmem],
        out_specs=(vmem,) * 4,
        scratch_shapes=[pltpu.VMEM((2 * BLOCK, GROUP * HEAD), jnp.bfloat16)],
        compiler_params=pltpu.CompilerParams(vmem_limit_bytes=16 * 1024 * 1024),
        name="merge",
    )(me, mine, theirs)


def join_kernel(me, *refs):
    out = refs[4]
    width = GROUP * HEAD
    for k in range(4):
        out[:, pl.ds(pl.multiple_of(lax.rem(me[0] + 4 - k, 4) * width, width), width)] = refs[k][...]


def join(me, parts):
    vmem = pl.BlockSpec(memory_space=pltpu.VMEM)
    return pl.pallas_call(
        join_kernel,
        out_shape=jax.ShapeDtypeStruct((parts[0].shape[0], 4 * GROUP * HEAD), jnp.bfloat16),
        in_specs=[pl.BlockSpec(memory_space=pltpu.SMEM)] + [vmem] * 4,
        out_specs=vmem,
        compiler_params=pltpu.CompilerParams(vmem_limit_bytes=8 * 1024 * 1024),
        name="join",
    )(me, *parts)


def spread_kernel(keys, values, out, near_keys, near_values, sems):
    copies = [
        pltpu.make_async_copy(keys, near_keys, sems.at[0]),
        pltpu.make_async_copy(values, near_values, sems.at[1]),
    ]
    for copy in copies:
        copy.start()
    for copy in copies:
        copy.wait()
    for h in range(KEY_VALUE_HEADS):
        sl = slice(h * HEAD, (h + 1) * HEAD)
        k, v = near_keys[:, sl], near_values[:, sl]
        for i in range(NX):
            out[i * KEY_VALUE_HEADS + h, :, 0:HEAD] = k
            out[i * KEY_VALUE_HEADS + h, :, HEAD : 2 * HEAD] = v


def spread(keys, values):
    return pl.pallas_call(
        spread_kernel,
        out_shape=jax.ShapeDtypeStruct((NX * KEY_VALUE_HEADS, keys.shape[0], 2 * HEAD), jnp.bfloat16),
        in_specs=[pl.BlockSpec(memory_space=pltpu.HBM)] * 2,
        out_specs=pl.BlockSpec(memory_space=pltpu.VMEM),
        scratch_shapes=[
            pltpu.VMEM(keys.shape, keys.dtype),
            pltpu.VMEM(values.shape, values.dtype),
            pltpu.SemaphoreType.DMA((2,)),
        ],
        compiler_params=pltpu.CompilerParams(vmem_limit_bytes=62 * 1024 * 1024),
        name="spread",
    )(keys, values)


def lookup(block_order, index):
    table = jnp.arange(block_order.shape[0], dtype=jnp.int32)
    return jnp.sum(jnp.where(index[:, None] == table[None, :], block_order[None, :], 0), axis=1)


def attention(queries, keys, values, block_order):
    rows = queries.shape[0]
    x, z, c = lax.axis_index("x"), lax.axis_index("z"), lax.axis_index("c")
    line = lax.all_to_all(spread(keys, values), ("x", "tp"), split_axis=0, concat_axis=0, tiled=True)
    line = line.reshape(-1, 2 * HEAD)

    q_own = lax.all_to_all(queries, "tp", split_axis=1, concat_axis=0, tiled=True)
    q_other = lax.ppermute(q_own, "c", shift(2, 1))

    ctx = (x * NZ + z) * 2
    own = np.asarray([1, 1, 0, 0], np.int32)
    core = own * c + (1 - own) * (1 - c)
    qpos = lookup(block_order, 2 * (ctx + core) + np.asarray([0, 1, 0, 1], np.int32))

    offsets = [(0, -1, 1), (-2, 2), (-3, 3), (NZ // 2,)]
    most = 2 * NX * max(len(o) for o in offsets)
    dz, dx, slot, real = (np.zeros((len(offsets), most), np.int32) for _ in range(4))
    for i, group in enumerate(offsets):
        for j, (o, xs, sl) in enumerate((o, xs, sl) for o in group for xs in range(NX) for sl in range(2)):
            dz[i, j], dx[i, j], slot[i, j], real[i, j] = o, xs, sl, 1
    stored = lookup(block_order, (2 * ((dx * NZ + (z + dz) % NZ) * 2 + c) + slot).reshape(-1)).reshape(dz.shape)
    tables = tables_of(qpos, jnp.where(real == 1, stored, 1 << 20))

    up, down = lax.ppermute(line, "z", shift(NZ, 1)), lax.ppermute(line, "z", shift(NZ, -1))
    pieces, state = [line, up, down], None
    for i in range(len(offsets)):
        if i < len(offsets) - 2:
            up, down = lax.ppermute(up, "z", shift(NZ, 1)), lax.ppermute(down, "z", shift(NZ, -1))
        elif i == len(offsets) - 2:
            half = line.shape[0] // 2
            up, down = lax.ppermute(up[:half], "z", shift(NZ, 1)), lax.ppermute(down[half:], "z", shift(NZ, -1))
        part = [t[i] for t in tables]
        if i < len(offsets) - 1:
            state = attend(part, qpos, (q_own, q_other), pieces, state)
            up, down, state = lax.optimization_barrier((up, down, state))
            pieces = [up, down]
    (sent,) = attend(part, qpos, (q_own, q_other), pieces, state, (1,))
    theirs = lax.ppermute(sent, "c", shift(2, 1))
    (mine,) = attend(part, qpos, (q_own, q_other), pieces, state, (0,))
    me = lax.axis_index("tp").reshape(1)
    parts = merge(me, mine, theirs, rows)
    parts = [parts[0]] + [lax.ppermute(parts[k], "tp", shift(4, k)) for k in range(1, 4)]
    return join(me, parts)


def solution(mesh):
    cut = Mesh(mesh.devices.reshape(NX, NZ, 2, 4), ("x", "z", "c", "tp"))
    placed = P(("x", "z", "c", "tp"), None)
    return jax.shard_map(attention, mesh=cut, in_specs=(placed, placed, placed, P()), out_specs=placed, check_vma=False)
```

```python
import functools
import math

import jax
import jax.numpy as jnp
import numpy as np
from jax import lax
from jax.experimental import pallas as pl
from jax.experimental.pallas import tpu as pltpu
from jax.sharding import Mesh, PartitionSpec as P


QUERY_HEAD_COUNT = 32
KEY_VALUE_HEADS = 4
HEAD = 128
GROUP = QUERY_HEAD_COUNT // KEY_VALUE_HEADS
BLOCK = 96
LANES = GROUP * BLOCK
TILE = 8
WIDE = 256
NEG = -1e30
LOG2_SCALE = HEAD ** -0.5 * math.log2(math.e)
TOO_LARGE = 2.0**60
ROWS = HEAD + 8
NX, NZ = 4, 8


def shift(n, k):
    return [(i, (i + k) % n) for i in range(n)]


def attend_kernel(counts, first, sides, *refs):
    cnt, seen, idx, kpos, qpos = refs[:5]
    at = 5 + len(sides)
    queries = refs[5:at]
    pieces = refs[at : at + len(counts)]
    at += len(counts)
    if not first:
        before = refs[at : at + len(sides)]
        at += len(sides)
    outs = refs[at : at + len(sides)]
    kv, q_turned, work = refs[at + len(sides) :]
    row = 0
    for piece, n in zip(pieces, counts):
        kv[row : row + n * BLOCK] = piece[...]
        row += n * BLOCK

    def fetch(qb, place, width):
        offs = [pl.multiple_of(idx[qb, place + j] * BLOCK, BLOCK) for j in range(width)]
        keys = jnp.concatenate([kv[pl.ds(f, BLOCK), 0:HEAD] for f in offs], 0)
        return keys, jnp.concatenate([kv[pl.ds(f, BLOCK), HEAD : 2 * HEAD] for f in offs], 0).T

    def pipelined(keys, mask, soften, weigh):
        chunks = LANES // WIDE

        def logits(c):
            s = jnp.dot(keys, q_turned[:, c * WIDE : (c + 1) * WIDE], preferred_element_type=jnp.float32)
            return mask(c, s)

        s, held = logits(0), None
        for c in range(chunks):
            following = logits(c + 1) if c + 1 < chunks else None
            now = soften(slice(c * WIDE, (c + 1) * WIDE), s)
            if held is not None:
                weigh(*held)
            held, s = now, following
        weigh(*held)

    def careful(qb, place):
        keys, vals = fetch(qb, place, 2)
        inner = lax.broadcasted_iota(jnp.int32, (BLOCK, 1), 0)
        kp = jnp.concatenate([inner + kpos[qb, place + j] * BLOCK for j in range(2)], 0)

        def mask(c, s):
            lane = lax.broadcasted_iota(jnp.int32, (1, WIDE), 1) + c * WIDE
            return jnp.where(kp <= lane % BLOCK + qpos[qb] * BLOCK, s, NEG)

        def soften(sl, s):
            top = work[HEAD : HEAD + 1, sl]
            new = jnp.maximum(top, jnp.max(s, 0, keepdims=True))
            p = jnp.exp2((s - new) * LOG2_SCALE)
            decay = jnp.exp2((top - new) * LOG2_SCALE)
            work[HEAD : HEAD + 1, sl] = new
            work[HEAD + 1 : HEAD + 2, sl] = work[HEAD + 1 : HEAD + 2, sl] * decay + jnp.sum(p, 0, keepdims=True)
            return sl, p.astype(jnp.bfloat16), decay

        def weigh(sl, p, decay):
            work[0:HEAD, sl] = work[0:HEAD, sl] * decay + jnp.dot(vals, p, preferred_element_type=jnp.float32)

        pipelined(keys, mask, soften, weigh)

    def quick(qb, place, width, left):
        keys, vals = fetch(qb, place, width)
        cut = (width - 1) * BLOCK

        def mask(c, s):
            if left is None:
                return s
            return jnp.concatenate([s[:cut], s[cut:] + jnp.where(left == width, 0.0, NEG)], 0)

        def soften(sl, s):
            p = jnp.exp2((s - work[HEAD : HEAD + 1, sl]) * LOG2_SCALE)
            work[HEAD + 1 : HEAD + 2, sl] += jnp.sum(p, 0, keepdims=True)
            return sl, p.astype(jnp.bfloat16)

        def weigh(sl, p):
            work[0:HEAD, sl] += jnp.dot(vals, p, preferred_element_type=jnp.float32)

        pipelined(keys, mask, soften, weigh)

    def query_block(b, carry):
        qb = 2 * sides[0] + b
        n = cnt[qb]
        lead = jnp.where((seen[qb] == 0) | (kpos[qb, 0] == qpos[qb]), jnp.minimum(n, 1), 0)
        full = lax.div(jnp.maximum(n - 2 * lead, 0), TILE)
        at = 2 * lead + full * TILE
        left = n - at

        def load():
            if first:
                work[0:HEAD] = jnp.zeros((HEAD, LANES), jnp.float32)
                work[HEAD : HEAD + 1] = jnp.full((1, LANES), NEG, jnp.float32)
                work[HEAD + 1 : ROWS] = jnp.zeros((ROWS - HEAD - 1, LANES), jnp.float32)
            else:
                for i in range(len(sides)):

                    @pl.when(b // 2 == i)
                    def _():
                        work[...] = before[i][b % 2]

        load()
        for i in range(len(sides)):

            @pl.when(b // 2 == i)
            def _():
                start = pl.multiple_of(b % 2 * BLOCK, BLOCK)
                heads = [queries[i][pl.ds(start, BLOCK), h * HEAD : (h + 1) * HEAD] for h in range(GROUP)]
                q_turned[...] = jnp.concatenate(heads, 0).T

        def slow(t, carry):
            careful(qb, t * 2)
            return carry

        def fast(t, carry):
            quick(qb, 2 * lead + t * TILE, TILE, None)
            return carry

        lax.fori_loop(0, lead, slow, 0)
        lax.fori_loop(0, full, fast, 0)
        for width in range(2, TILE + 1, 2):

            @pl.when((left == width) | (left == width - 1))
            def _():
                quick(qb, at, width, left)

        fine = jnp.max(jnp.where(work[HEAD + 1 : HEAD + 2] < TOO_LARGE, 0.0, 1.0)) == 0.0

        @pl.when(jnp.logical_not(fine))
        def _():
            load()
            lax.fori_loop(0, lax.div(n + 1, 2), slow, 0)

        for i in range(len(sides)):

            @pl.when(b // 2 == i)
            def _():
                outs[i][b % 2] = work[...]

        return carry

    lax.fori_loop(0, 2 * len(sides), query_block, 0)


def attend(tables, qpos, queries, pieces, state, sides=(0, 1)):
    counts = [p.shape[0] // BLOCK for p in pieces]
    total = sum(counts)
    first = state is None
    smem = pl.BlockSpec(memory_space=pltpu.SMEM)
    vmem = pl.BlockSpec(memory_space=pltpu.VMEM)
    held = [] if first else [state[i] for i in sides]
    shape = jax.ShapeDtypeStruct((2, ROWS, LANES), jnp.float32)
    return pl.pallas_call(
        functools.partial(attend_kernel, counts, first, sides),
        out_shape=(shape,) * len(sides),
        in_specs=[smem] * 5 + [vmem] * len(sides) + [vmem] * len(pieces) + [vmem] * len(held),
        out_specs=(vmem,) * len(sides),
        scratch_shapes=[
            pltpu.VMEM((total * BLOCK, 2 * HEAD), jnp.bfloat16),
            pltpu.VMEM((HEAD, LANES), jnp.bfloat16),
            pltpu.VMEM((ROWS, LANES), jnp.float32),
        ],
        compiler_params=pltpu.CompilerParams(vmem_limit_bytes=32 * 1024 * 1024),
        cost_estimate=pl.CostEstimate(
            flops=total * len(sides) * LANES * BLOCK * HEAD * 4,
            bytes_accessed=total * BLOCK * 4 * HEAD + 4 * ROWS * LANES * 4,
            transcendentals=total * len(sides) * LANES * BLOCK,
        ),
        name="attend",
    )(*tables, qpos, *[queries[i] for i in sides], *pieces, *held)


def tables_of(qblk, kblk):
    nb = kblk.shape[1]
    here = jnp.arange(nb, dtype=jnp.int32)
    k, q = kblk[:, None, :], qblk[None, :, None]
    rank = jnp.where(k <= q, jnp.where(k == q, -1, here), 2 * nb + here)
    place = jnp.sum(rank[:, :, None, :] < rank[:, :, :, None], 3)
    hit = place[:, :, :, None] == here
    idx = jnp.sum(jnp.where(hit, here[:, None], 0), 2).astype(jnp.int32)
    kpos = jnp.sum(jnp.where(hit, k[:, :, :, None], 0), 2).astype(jnp.int32)
    cnt = jnp.sum(k <= q, 2).astype(jnp.int32)
    return cnt, jnp.cumsum(cnt, 0) - cnt, idx, kpos


def merge_kernel(me, mine, theirs, *refs):
    outs, rows_ref = refs[:4], refs[4]
    for b in range(2):
        m1, m2 = mine[b, HEAD : HEAD + 1], theirs[b, HEAD : HEAD + 1]
        top = jnp.maximum(m1, m2)
        w1 = jnp.exp2((m1 - top) * LOG2_SCALE)
        w2 = jnp.exp2((m2 - top) * LOG2_SCALE)
        denom = mine[b, HEAD + 1 : HEAD + 2] * w1 + theirs[b, HEAD + 1 : HEAD + 2] * w2
        o = (mine[b, 0:HEAD] * w1 + theirs[b, 0:HEAD] * w2) / denom
        rows = o.T.astype(jnp.bfloat16)
        for h in range(GROUP):
            rows_ref[b * BLOCK : (b + 1) * BLOCK, h * HEAD : (h + 1) * HEAD] = rows[h * BLOCK : (h + 1) * BLOCK]
    count = outs[0].shape[0]
    for k, out in enumerate(outs):
        out[...] = rows_ref[pl.ds(pl.multiple_of(lax.rem(me[0] + k, 4) * count, count), count)]


def merge(me, mine, theirs, rows):
    vmem = pl.BlockSpec(memory_space=pltpu.VMEM)
    return pl.pallas_call(
        merge_kernel,
        out_shape=(jax.ShapeDtypeStruct((rows, GROUP * HEAD), jnp.bfloat16),) * 4,
        in_specs=[pl.BlockSpec(memory_space=pltpu.SMEM), vmem, vmem],
        out_specs=(vmem,) * 4,
        scratch_shapes=[pltpu.VMEM((2 * BLOCK, GROUP * HEAD), jnp.bfloat16)],
        compiler_params=pltpu.CompilerParams(vmem_limit_bytes=16 * 1024 * 1024),
        name="merge",
    )(me, mine, theirs)


def join_kernel(me, *refs):
    out = refs[4]
    width = GROUP * HEAD
    for k in range(4):
        out[:, pl.ds(pl.multiple_of(lax.rem(me[0] + 4 - k, 4) * width, width), width)] = refs[k][...]


def join(me, parts):
    vmem = pl.BlockSpec(memory_space=pltpu.VMEM)
    return pl.pallas_call(
        join_kernel,
        out_shape=jax.ShapeDtypeStruct((parts[0].shape[0], 4 * GROUP * HEAD), jnp.bfloat16),
        in_specs=[pl.BlockSpec(memory_space=pltpu.SMEM)] + [vmem] * 4,
        out_specs=vmem,
        compiler_params=pltpu.CompilerParams(vmem_limit_bytes=8 * 1024 * 1024),
        name="join",
    )(me, *parts)


def spread_kernel(keys, values, out, near_keys, near_values, sems):
    copies = [
        pltpu.make_async_copy(keys, near_keys, sems.at[0]),
        pltpu.make_async_copy(values, near_values, sems.at[1]),
    ]
    for copy in copies:
        copy.start()
    for copy in copies:
        copy.wait()
    for h in range(KEY_VALUE_HEADS):
        sl = slice(h * HEAD, (h + 1) * HEAD)
        k, v = near_keys[:, sl], near_values[:, sl]
        for i in range(NX):
            out[i * KEY_VALUE_HEADS + h, :, 0:HEAD] = k
            out[i * KEY_VALUE_HEADS + h, :, HEAD : 2 * HEAD] = v


def spread(keys, values):
    return pl.pallas_call(
        spread_kernel,
        out_shape=jax.ShapeDtypeStruct((NX * KEY_VALUE_HEADS, keys.shape[0], 2 * HEAD), jnp.bfloat16),
        in_specs=[pl.BlockSpec(memory_space=pltpu.HBM)] * 2,
        out_specs=pl.BlockSpec(memory_space=pltpu.VMEM),
        scratch_shapes=[
            pltpu.VMEM(keys.shape, keys.dtype),
            pltpu.VMEM(values.shape, values.dtype),
            pltpu.SemaphoreType.DMA((2,)),
        ],
        compiler_params=pltpu.CompilerParams(vmem_limit_bytes=62 * 1024 * 1024),
        name="spread",
    )(keys, values)


def lookup(block_order, index):
    table = jnp.arange(block_order.shape[0], dtype=jnp.int32)
    return jnp.sum(jnp.where(index[:, None] == table[None, :], block_order[None, :], 0), axis=1)


def attention(queries, keys, values, block_order):
    rows = queries.shape[0]
    x, z, c = lax.axis_index("x"), lax.axis_index("z"), lax.axis_index("c")
    line = lax.all_to_all(spread(keys, values), ("x", "tp"), split_axis=0, concat_axis=0, tiled=True)
    line = line.reshape(-1, 2 * HEAD)

    ctx = (x * NZ + z) * 2
    own = np.asarray([1, 1, 0, 0], np.int32)
    core = own * c + (1 - own) * (1 - c)
    qpos = lookup(block_order, 2 * (ctx + core) + np.asarray([0, 1, 0, 1], np.int32))

    offsets = [(0, -1), (1, -2, 2), (-3, 3), (NZ // 2,)]
    most = 2 * NX * max(len(o) for o in offsets)
    dz, dx, slot, real = (np.zeros((len(offsets), most), np.int32) for _ in range(4))
    for i, group in enumerate(offsets):
        for j, (o, xs, sl) in enumerate((o, xs, sl) for o in group for xs in range(NX) for sl in range(2)):
            dz[i, j], dx[i, j], slot[i, j], real[i, j] = o, xs, sl, 1
    stored = lookup(block_order, (2 * ((dx * NZ + (z + dz) % NZ) * 2 + c) + slot).reshape(-1)).reshape(dz.shape)
    tables = tables_of(qpos, jnp.where(real == 1, stored, 1 << 20))
    queries, *tables = lax.optimization_barrier((queries, *tables))

    q_own = lax.all_to_all(queries, "tp", split_axis=1, concat_axis=0, tiled=True)
    q_other = lax.ppermute(q_own, "c", shift(2, 1))

    up, down = lax.ppermute(line, "z", shift(NZ, 1)), lax.ppermute(line, "z", shift(NZ, -1))
    pieces, state = [line, up], None
    later = [down]
    for i in range(len(offsets)):
        if i < len(offsets) - 2:
            up, down = lax.ppermute(up, "z", shift(NZ, 1)), lax.ppermute(down, "z", shift(NZ, -1))
        elif i == len(offsets) - 2:
            half = line.shape[0] // 2
            up, down = lax.ppermute(up[:half], "z", shift(NZ, 1)), lax.ppermute(down[half:], "z", shift(NZ, -1))
        part = [t[i] for t in tables]
        if i < len(offsets) - 1:
            state = attend(part, qpos, (q_own, q_other), pieces, state)
            up, down, state = lax.optimization_barrier((up, down, state))
            pieces, later = later + [up, down], []
    (sent,) = attend(part, qpos, (q_own, q_other), pieces, state, (1,))
    theirs = lax.ppermute(sent, "c", shift(2, 1))
    (mine,) = attend(part, qpos, (q_own, q_other), pieces, state, (0,))
    me = lax.axis_index("tp").reshape(1)
    parts = merge(me, mine, theirs, rows)
    parts = [parts[0]] + [lax.ppermute(parts[k], "tp", shift(4, k)) for k in range(1, 4)]
    return join(me, parts)


def solution(mesh):
    cut = Mesh(mesh.devices.reshape(NX, NZ, 2, 4), ("x", "z", "c", "tp"))
    placed = P(("x", "z", "c", "tp"), None)
    return jax.shard_map(attention, mesh=cut, in_specs=(placed, placed, placed, P()), out_specs=placed, check_vma=False)
```
